32 devices in a mesh: row: 8 (over z, core), col: 4 (over y, x).
Axes of the slice: x: 2, y: 2, z: 4, core: 2. Of those that a mesh axis runs over, the one named last changes fastest.
Arguments:
- queries: bfloat16 [32768, 256], P(('row', 'col')), may hold values from -6 to 6
- documents: bfloat16 [1024, 256], P(('row', 'col')), may hold values from -6 to 6
- log_norms: float32 [32768], P(('row', 'col')), may hold values from 7 to 11
- weights: float32 [32768], P(('row', 'col')), may hold values from 1 to 10
- positives: int32 [32768], P(('row', 'col')), may hold values from 0 to 1023
Outputs:
- grad_queries: bfloat16 [32768, 256], P(('row', 'col'))
- grad_documents: bfloat16 [1024, 256], P(('row', 'col'))
- loss: float32 [], replicated
The draws below stay inside these ranges and needn't reach their ends.
All inputs are finite; a program needn't handle non-finite values.
Results may differ from the reference program's by a relative error of at most 0.001.
The reference program's roundings to bfloat16 on the way (of `coeffs`) count: a program that leaves them out, or rounds other values in their place, can miss the bound.
Values may be sent and summed in bfloat16 or wider, within the bound.
A program may use at most 128 MiB of HBM per device.

```python
import math
import jax
import jax.numpy as jnp
from jax import lax

E = 256
NQ = 32768
ND = 1024


def set_ends(drawn, own_key, smallest, largest):
    dims = drawn.shape
    spot = [jax.random.randint(jax.random.fold_in(own_key, axis), (), 0, dims[axis]) for axis in range(len(dims))]
    drawn = drawn.at[tuple(spot)].set(smallest)
    longest = dims.index(max(dims))
    spot[longest] = (spot[longest] + 1) % dims[longest]
    return drawn.at[tuple(spot)].set(largest)


def levels(rng, extent, split, least, largest):
    def one(axis_at, parts):
        draws = jax.random.uniform(jax.random.fold_in(jax.random.fold_in(rng, 6), axis_at), (parts,), jnp.float32, least / len(split), largest / len(split))
        return jnp.repeat(jnp.exp(draws), extent[axis_at] // parts).reshape((-1,) + (1,) * (len(extent) - axis_at - 1))

    loudness = one(*split[0])
    for cut in split[1:]:
        loudness = loudness * one(*cut)
    return loudness


def noise(key, extent, deviation, most, pieces=(), kind=jnp.bfloat16):
    entries = deviation * jax.random.normal(key, extent, jnp.float32)
    if pieces:
        entries = entries * levels(key, extent, pieces, -0.22, 0.18)
    return jnp.clip(entries, -most, most).astype(kind)


def setup_inputs(seed: int = 0) -> dict:
    arg_keys = jax.random.split(jax.random.key(seed), 6)
    return {
        "queries": noise(arg_keys[0], (NQ, E), 1.0, 6.0, ((0, 32),)),
        "documents": noise(arg_keys[1], (ND, E), 1.0, 6.0, ((0, 32),)),
        "log_norms": jnp.clip(7.0 + 4.0 * jax.random.uniform(arg_keys[2], (NQ,), jnp.float32) ** levels(arg_keys[2], (NQ,), ((0, 32),), -0.2, 0.2), 7.0, 11.0),
        "weights": jnp.clip(jnp.exp(math.log(10.0) - 2.3025851 * jax.random.uniform(arg_keys[3], (NQ,), jnp.float32) ** levels(arg_keys[3], (NQ,), ((0, 32),), -0.2, 0.2)), 1.0, 10.0),
        "positives": set_ends(jax.random.randint(arg_keys[4], (NQ,), 0, ND), jax.random.fold_in(arg_keys[4], 1), 0, ND - 1).astype(jnp.int32),
    }


def reference(queries, documents, log_norms, weights, positives):
    num_q = queries.shape[0]
    num_d = documents.shape[0]
    width = queries.shape[1]
    qblock = math.gcd(num_q, 1024)
    nblocks = num_q // qblock
    doc_ids = jnp.arange(num_d, dtype=jnp.int32)

    def visit(acc, items):
        qrows, lse, wts, pos = items
        scores = jnp.dot(qrows, documents.T, preferred_element_type=jnp.float32) * 0.0625
        probs = jnp.exp(scores - lse[:, None])
        hits = (pos[:, None] == doc_ids[None, :]).astype(jnp.float32)
        pos_scores = jnp.sum(hits * scores, axis=1)
        coeffs = ((probs - hits) * wts[:, None]).astype(jnp.bfloat16)
        grad_q = jnp.dot(coeffs, documents, preferred_element_type=jnp.float32) * 0.0625
        acc = acc + lax.dot_general(coeffs, qrows, (((0,), (0,)), ((), ())), preferred_element_type=jnp.float32)
        part = jnp.sum(wts * (lse - pos_scores))
        return acc, (grad_q.astype(jnp.bfloat16), part)

    items = (queries.reshape(nblocks, qblock, width), log_norms.reshape(nblocks, qblock),
             weights.reshape(nblocks, qblock), positives.reshape(nblocks, qblock))
    acc, outs = lax.scan(visit, jnp.zeros((num_d, width), jnp.float32), items)
    grad_queries = outs[0].reshape(num_q, width)
    grad_documents = (acc * 0.0625).astype(jnp.bfloat16)
    loss = jnp.sum(outs[1]) / num_q
    return grad_queries, grad_documents, loss
```

```python
import functools
import math

import jax
import jax.numpy as jnp
from jax import lax
from jax.experimental import pallas as pl
from jax.experimental.pallas import tpu as pltpu
from jax.sharding import PartitionSpec as P

MESH = pl.DeviceIdType.MESH
LOG2E = math.log2(math.e)
F32 = jnp.float32
BF16 = jnp.bfloat16


def flipped(index, step, size):
    total, bit = 0, 1
    while bit < size:
        own = (index // bit) % 2
        other = (step // bit) % 2
        total = total + bit * ((own + other) % 2)
        bit *= 2
    return total


def tree_sum(parts):
    while len(parts) > 1:
        parts = [parts[i] + parts[i + 1] for i in range(0, len(parts), 2)]
    return parts[0]


def kernel(
    n_row, n_col, nd_own, total_q,
    q_hbm, d_hbm, ln_ref, w_ref, pos_ref,
    gq_ref, gd_ref, loss_ref,
    q, q_t, docs, coeffs, part, recv1, recv2, recv3, bias,
    loss_own, loss_in1, loss_in2, loss_in3,
    local_sem, s_z, r_z, s_p, r_p, s_c, r_c, s_f, r_f,
    s_1, r_1, s_2, r_2, s_3, r_3, s_l, r_l,
):
    chips = n_row // 2
    row = lax.axis_index("row")
    col = lax.axis_index("col")
    core = row % 2
    chip = row // 2
    nq, width = q.shape
    half = chips * nd_own
    block = 2 * half

    partner = (chip * 2 + (1 - core), col)
    along_row = [None] + [(flipped(chip, t, chips) * 2 + core, col) for t in range(1, chips)]
    along_col = [None] + [(row, flipped(col, s, n_col)) for s in range(1, n_col)]

    get_d = pltpu.make_async_copy(d_hbm, docs.at[pl.ds(0, nd_own)], local_sem.at[0])
    get_d.start()
    get_q = pltpu.make_async_copy(q_hbm, q, local_sem.at[1])
    get_q.start()

    barrier = pltpu.get_barrier_semaphore()
    peers = [partner] + along_row[1:] + along_col[1:]
    for peer in peers:
        pl.semaphore_signal(barrier, inc=1, device_id=peer, device_id_type=MESH)
    get_d.wait()
    pl.semaphore_wait(barrier, len(peers))

    def send(src, dst, s_sem, r_sem, peer):
        return pltpu.make_async_remote_copy(
            src_ref=src, dst_ref=dst, send_sem=s_sem, recv_sem=r_sem,
            device_id=peer, device_id_type=MESH,
        )

    def piece(s, k, t, count=1):
        return docs.at[pl.ds(s * block + k * half + t * nd_own, count * nd_own)]

    started = []

    def go(copy):
        copy.start()
        started.append(copy)
        return copy

    z_copies = [None]
    for t in range(1, chips):
        z_copies.append(go(send(piece(0, 0, 0), piece(0, 0, t), s_z.at[t], r_z.at[t], along_row[t])))
    for t in range(chips):
        if t:
            z_copies[t].wait_recv()
        for s in range(1, n_col):
            send(piece(0, 0, t), piece(s, 0, t), s_c.at[s], r_c.at[s], along_col[s]).start()
        if t == 0:
            bias[...] = ln_ref[...] * LOG2E - jnp.log2(w_ref[...])
            get_q.wait()
            q_t[...] = q[...].T
    own_fwd = [
        go(send(piece(0, 0, 0, chips), piece(0, 1, 0, chips), s_f.at[0], r_f.at[0], partner))
    ]

    rows_per = math.gcd(block, 256)
    pieces = rows_per // nd_own
    iota = lax.broadcasted_iota(jnp.int32, (nd_own, nq), 0)

    def scores_of(s, sub, acc):
        base = pl.multiple_of(s * block + sub * rows_per, rows_per)
        d = docs[pl.ds(base, rows_per), :]
        sc = jnp.dot(d, q_t[...], preferred_element_type=F32)
        other_col = flipped(col, s, n_col)
        for p in range(pieces):
            at = sub * pieces + p
            k, t = at // chips, at % chips
            owner_row = flipped(chip, t, chips) * 2 + (core + k) % 2
            first = (owner_row * n_col + other_col) * nd_own
            x = sc[p * nd_own:(p + 1) * nd_own, :]
            hit_w = jnp.where(pos_ref[...] - first == iota, w_ref[...], 0.0)
            co = jnp.exp2(x * (0.0625 * LOG2E) - bias[...]) - hit_w
            coeffs[pl.ds(base + p * nd_own, nd_own), :] = co.astype(BF16)
            acc = acc + hit_w * x
        part[pl.ds(base, rows_per), :] = jnp.dot(
            coeffs[pl.ds(base, rows_per), :], q[...], preferred_element_type=F32
        )
        return acc

    n_sub = block // rows_per
    hit_sum = jnp.zeros((nd_own, nq), F32)
    firsts = []

    def own_half(s):
        return part.at[pl.ds(s * block, half)]

    def reduce_pair(s):
        firsts[s].wait_recv()
        own = pl.ds(s * block, half)
        part[own, :] = part[own, :] + recv1[pl.ds(s * half, half), :]
        if s:
            seconds.append(
                go(send(own_half(s), recv2.at[pl.ds(s * half, half)], s_2.at[s], r_2.at[s], along_col[s]))
            )

    seconds = [None]
    fwd = own_fwd
    for s in range(n_col):
        if s:
            whole = send(piece(0, 0, 0, chips), piece(s, 0, 0, chips), s_c.at[s], r_c.at[s], along_col[s])
            whole.wait_recv()
            fwd.append(
                go(send(piece(s, 0, 0, chips), piece(s, 1, 0, chips), s_f.at[s], r_f.at[s], partner))
            )
        fwd[s].wait_recv()
        if n_sub == 1:
            hit_sum = scores_of(s, 0, hit_sum)
        else:
            hit_sum = lax.fori_loop(0, n_sub, functools.partial(scores_of, s), hit_sum)
        firsts.append(
            go(send(
                part.at[pl.ds(s * block + half, half)], recv1.at[pl.ds(s * half, half)],
                s_1.at[s], r_1.at[s], partner,
            ))
        )
        if s:
            reduce_pair(s - 1)

    terms = w_ref[...] * ln_ref[...] - 0.0625 * jnp.sum(hit_sum, axis=0, keepdims=True)
    loss_own[0] = jnp.broadcast_to(jnp.sum(terms, axis=1, keepdims=True), (8, 128))
    l1 = go(send(loss_own.at[0], loss_in1.at[1], s_l.at[0], r_l.at[0], partner))
    reduce_pair(n_col - 1)
    l1.wait_recv()
    loss_own[1] = loss_own[0] + loss_in1[1]
    l2 = [go(send(loss_own.at[1], loss_in2.at[s], s_l.at[s], r_l.at[s], along_col[s])) for s in range(1, n_col)]

    d_t = docs[...].T
    chunk = math.gcd(nq, 256)
    n_chunks = nq // chunk

    def query_gradient(j):
        at = slice(j * chunk, (j + 1) * chunk)
        g = jnp.dot(d_t, coeffs[:, at], preferred_element_type=F32)
        gq_ref[at, :] = (g.T * 0.0625).astype(BF16)

    for j in range(n_chunks):
        query_gradient(j)

    own = pl.ds(0, half)
    for s in range(1, n_col):
        seconds[s].wait_recv()
        part[own, :] = part[own, :] + recv2[pl.ds(s * half, half), :]
    thirds = [None] + [
        go(send(
            part.at[pl.ds(t * nd_own, nd_own)], recv3.at[pl.ds(t * nd_own, nd_own)],
            s_3.at[t], r_3.at[t], along_row[t],
        ))
        for t in range(1, chips)
    ]
    for c in l2:
        c.wait_recv()
    loss_own[2] = tree_sum([loss_own[1]] + [loss_in2[s] for s in range(1, n_col)])
    l3 = [
        go(send(loss_own.at[2], loss_in3.at[t], s_l.at[n_col + t], r_l.at[n_col + t], along_row[t]))
        for t in range(1, chips)
    ]
    total = part[pl.ds(0, nd_own), :]
    for t in range(1, chips):
        thirds[t].wait_recv()
        total = total + recv3[pl.ds(t * nd_own, nd_own), :]
    gd_ref[...] = (total * 0.0625).astype(BF16)
    for c in l3:
        c.wait_recv()
    final = tree_sum([loss_own[2]] + [loss_in3[t] for t in range(1, chips)])
    loss_ref[...] = final * (1.0 / total_q)

    for s in range(1, n_col):
        send(piece(0, 0, 0, chips), piece(s, 0, 0, chips), s_c.at[s], r_c.at[s], along_col[s]).wait_send()
    for copy in started:
        copy.wait_send()


def on_device(queries, documents, log_norms, weights, positives):
    n_row = lax.axis_size("row")
    n_col = lax.axis_size("col")
    nq, width = queries.shape
    nd_own = documents.shape[0]
    chips = n_row // 2
    nd = nd_own * n_row * n_col
    half = chips * nd_own
    sem = pltpu.SemaphoreType.DMA
    vmem = pl.BlockSpec(memory_space=pltpu.VMEM)
    hbm = pl.BlockSpec(memory_space=pl.ANY)
    gq, gd, loss = pl.pallas_call(
        functools.partial(kernel, n_row, n_col, nd_own, nq * n_row * n_col),
        out_shape=(
            jax.ShapeDtypeStruct((nq, width), BF16),
            jax.ShapeDtypeStruct((nd_own, width), BF16),
            jax.ShapeDtypeStruct((8, 128), F32),
        ),
        in_specs=[hbm, hbm, vmem, vmem, vmem],
        out_specs=(vmem, vmem, vmem),
        scratch_shapes=[
            pltpu.VMEM((nq, width), BF16),
            pltpu.VMEM((width, nq), BF16),
            pltpu.VMEM((nd, width), BF16),
            pltpu.VMEM((nd, nq), BF16),
            pltpu.VMEM((nd, width), F32),
            pltpu.VMEM((n_col * half, width), F32),
            pltpu.VMEM((n_col * half, width), F32),
            pltpu.VMEM((half, width), F32),
            pltpu.VMEM((1, nq), F32),
            pltpu.VMEM((3, 8, 128), F32),
            pltpu.VMEM((2, 8, 128), F32),
            pltpu.VMEM((n_col, 8, 128), F32),
            pltpu.VMEM((chips, 8, 128), F32),
            sem((2,)),
            sem((chips,)), sem((chips,)),
            sem((1,)), sem((1,)),
            sem((n_col,)), sem((n_col,)),
            sem((n_col,)), sem((n_col,)),
            sem((n_col,)), sem((n_col,)),
            sem((n_col,)), sem((n_col,)),
            sem((chips,)), sem((chips,)),
            sem((n_col + chips,)), sem((n_col + chips,)),
        ],
        compiler_params=pltpu.CompilerParams(
            collective_id=0, has_side_effects=True, vmem_limit_bytes=60 * 1024 * 1024
        ),
    )(
        queries, documents,
        log_norms.reshape(1, nq), weights.reshape(1, nq), positives.reshape(1, nq),
    )
    return (gq, gd, loss[0, 0])


def solution(mesh):
    placed = (
        P(("row", "col"), None),
        P(("row", "col"), None),
        P(("row", "col")),
        P(("row", "col")),
        P(("row", "col")),
    )
    return jax.shard_map(
        on_device,
        mesh=mesh,
        in_specs=placed,
        out_specs=(P(("row", "col"), None), P(("row", "col"), None), P()),
        check_vma=False,
    )
```

```python
import functools
import math

import jax
import jax.numpy as jnp
from jax import lax
from jax.experimental import pallas as pl
from jax.experimental.pallas import tpu as pltpu
from jax.sharding import PartitionSpec as P

MESH = pl.DeviceIdType.MESH
LOG2E = math.log2(math.e)
F32 = jnp.float32
BF16 = jnp.bfloat16


def flipped(index, step, size):
    total, bit = 0, 1
    while bit < size:
        own = (index // bit) % 2
        other = (step // bit) % 2
        total = total + bit * ((own + other) % 2)
        bit *= 2
    return total


def tree_sum(parts):
    while len(parts) > 1:
        parts = [parts[i] + parts[i + 1] for i in range(0, len(parts), 2)]
    return parts[0]


def kernel(
    n_row, n_col, nd_own, total_q,
    q_hbm, d_hbm, ln_ref, w_ref, pos_ref,
    gq_ref, gd_ref, loss_ref,
    q, q_t, docs, coeffs, part, recv1, recv2, recv3, bias,
    loss_own, loss_in1, loss_in2, loss_in3,
    local_sem, s_z, r_z, s_c, r_c, s_f, r_f,
    s_1, r_1, s_2, r_2, s_3, r_3, s_l, r_l,
):
    chips = n_row // 2
    row = lax.axis_index("row")
    col = lax.axis_index("col")
    core = row % 2
    chip = row // 2
    nq, width = q.shape
    half = n_col * nd_own
    block = 2 * half

    partner = (chip * 2 + (1 - core), col)
    along_row = [None] + [(flipped(chip, t, chips) * 2 + core, col) for t in range(1, chips)]
    along_col = [None] + [(row, flipped(col, s, n_col)) for s in range(1, n_col)]

    get_d = pltpu.make_async_copy(d_hbm, docs.at[pl.ds(0, nd_own)], local_sem.at[0])
    get_d.start()
    get_q = pltpu.make_async_copy(q_hbm, q, local_sem.at[1])
    get_q.start()

    barrier = pltpu.get_barrier_semaphore()
    peers = [partner] + along_row[1:] + along_col[1:]
    for peer in peers:
        pl.semaphore_signal(barrier, inc=1, device_id=peer, device_id_type=MESH)
    get_d.wait()
    pl.semaphore_wait(barrier, len(peers))

    def send(src, dst, s_sem, r_sem, peer):
        return pltpu.make_async_remote_copy(
            src_ref=src, dst_ref=dst, send_sem=s_sem, recv_sem=r_sem,
            device_id=peer, device_id_type=MESH,
        )

    def piece(t, k, s, count=1):
        return docs.at[pl.ds(t * block + k * half + s * nd_own, count * nd_own)]

    started = []

    def go(copy):
        copy.start()
        started.append(copy)
        return copy

    def from_row(t):
        return send(piece(0, 0, 0), piece(t, 0, 0), s_z.at[t], r_z.at[t], along_row[t])

    def over_col(t):
        for s in range(1, n_col):
            send(piece(t, 0, 0), piece(t, 0, s), s_c.at[t], r_c.at[t], along_col[s]).start()

    def all_over_col(t):
        others = piece(t, 0, 1, n_col - 1)
        return send(others, others, s_c.at[t], r_c.at[t], along_col[1])

    fwd = {}

    def to_partner(t):
        all_over_col(t).wait_recv()
        fwd[t] = go(send(piece(t, 0, 0, n_col), piece(t, 1, 0, n_col), s_f.at[t], r_f.at[t], partner))

    order = [0] + list(range(chips - 1, 0, -1))
    for t in order[1:]:
        go(from_row(t))
    over_col(0)
    bias[...] = ln_ref[...] * LOG2E - jnp.log2(w_ref[...])
    get_q.wait()
    q_t[...] = q[...].T
    to_partner(0)
    for t in order[1:]:
        from_row(t).wait_recv()
        over_col(t)

    rows_per = math.gcd(block, 256)
    pieces = rows_per // nd_own
    n_sub = block // rows_per
    iota = lax.broadcasted_iota(jnp.int32, (nd_own, nq), 0)

    def scores_of(t, sub, acc):
        base = pl.multiple_of(t * block + sub * rows_per, rows_per)
        d = docs[pl.ds(base, rows_per), :]
        sc = jnp.dot(d, q_t[...], preferred_element_type=F32)
        owner_chip = flipped(chip, t, chips)
        for p in range(pieces):
            at = sub * pieces + p
            k, s = at // n_col, at % n_col
            owner_row = owner_chip * 2 + (core + k) % 2
            first = (owner_row * n_col + flipped(col, s, n_col)) * nd_own
            x = sc[p * nd_own:(p + 1) * nd_own, :]
            hit_w = jnp.where(pos_ref[...] - first == iota, w_ref[...], 0.0)
            co = jnp.exp2(x * (0.0625 * LOG2E) - bias[...]) - hit_w
            coeffs[pl.ds(base + p * nd_own, nd_own), :] = co.astype(BF16)
            acc = acc + hit_w * x
        part[pl.ds(base, rows_per), :] = jnp.dot(
            coeffs[pl.ds(base, rows_per), :], q[...], preferred_element_type=F32
        )
        return acc

    def pair_copy(t):
        return send(
            part.at[pl.ds(t * block + half, half)], recv1.at[pl.ds(t * half, half)],
            s_1.at[t], r_1.at[t], partner,
        )

    def reduce_pair(t):
        pair_copy(t).wait_recv()
        own = pl.ds(t * block, half)
        part[own, :] = part[own, :] + recv1[pl.ds(t * half, half), :]
        for s in range(1, n_col):
            send(
                part.at[pl.ds(t * block + s * nd_own, nd_own)],
                recv2.at[pl.ds(t * half + s * nd_own, nd_own)],
                s_2.at[t], r_2.at[t], along_col[s],
            ).start()

    def all_col_sums(t):
        rest = (n_col - 1) * nd_own
        return send(
            part.at[pl.ds(t * block + nd_own, rest)],
            recv2.at[pl.ds(t * half + nd_own, rest)],
            s_2.at[t], r_2.at[t], along_col[1],
        )

    def row_copy(t):
        return send(
            part.at[pl.ds(t * block, nd_own)], recv3.at[pl.ds(t * nd_own, nd_own)],
            s_3.at[t], r_3.at[t], along_row[t],
        )

    def reduce_col(t):
        all_col_sums(t).wait_recv()
        total = part[pl.ds(t * block, nd_own), :]
        for s in range(1, n_col):
            total = total + recv2[pl.ds(t * half + s * nd_own, nd_own), :]
        part[pl.ds(t * block, nd_own), :] = total
        if t:
            go(row_copy(t))

    hit_sum = jnp.zeros((nd_own, nq), F32)
    for i, t in enumerate(order):
        fwd[t].wait_recv()
        if i + 1 < chips and i == 0:
            to_partner(order[1])
        if n_sub == 1:
            hit_sum = scores_of(t, 0, hit_sum)
        else:
            hit_sum = lax.fori_loop(0, n_sub, functools.partial(scores_of, t), hit_sum)
        go(pair_copy(t))
        if i + 2 < chips:
            to_partner(order[i + 2])
        if i >= 1:
            reduce_pair(order[i - 1])
        if i >= 2:
            reduce_col(order[i - 2])

    terms = w_ref[...] * ln_ref[...] - 0.0625 * jnp.sum(hit_sum, axis=0, keepdims=True)
    loss_own[0] = jnp.broadcast_to(jnp.sum(terms, axis=1, keepdims=True), (8, 128))
    l1 = go(send(loss_own.at[0], loss_in1.at[1], s_l.at[0], r_l.at[0], partner))

    d_t = docs[...].T
    chunk = math.gcd(nq, 256)
    n_chunks = nq // chunk

    def query_gradient(j):
        at = slice(j * chunk, (j + 1) * chunk)
        g = jnp.dot(d_t, coeffs[:, at], preferred_element_type=F32)
        gq_ref[at, :] = (g.T * 0.0625).astype(BF16)

    reduce_pair(order[-1])
    l1.wait_recv()
    loss_own[1] = loss_own[0] + loss_in1[1]
    l2 = [go(send(loss_own.at[1], loss_in2.at[s], s_l.at[s], r_l.at[s], along_col[s])) for s in range(1, n_col)]
    if chips > 1:
        reduce_col(order[-2])
    for j in range(n_chunks):
        query_gradient(j)
    reduce_col(order[-1])
    for c in l2:
        c.wait_recv()
    loss_own[2] = tree_sum([loss_own[1]] + [loss_in2[s] for s in range(1, n_col)])
    l3 = [
        go(send(loss_own.at[2], loss_in3.at[t], s_l.at[n_col + t], r_l.at[n_col + t], along_row[t]))
        for t in range(1, chips)
    ]
    total = part[pl.ds(0, nd_own), :]
    for t in order[1:]:
        row_copy(t).wait_recv()
        total = total + recv3[pl.ds(t * nd_own, nd_own), :]
    gd_ref[...] = (total * 0.0625).astype(BF16)
    for c in l3:
        c.wait_recv()
    final = tree_sum([loss_own[2]] + [loss_in3[t] for t in range(1, chips)])
    loss_ref[...] = final * (1.0 / total_q)

    for t in range(chips):
        all_over_col(t).wait_send()
        all_col_sums(t).wait_send()
    for copy in started:
        copy.wait_send()


def on_device(queries, documents, log_norms, weights, positives):
    n_row = lax.axis_size("row")
    n_col = lax.axis_size("col")
    nq, width = queries.shape
    nd_own = documents.shape[0]
    chips = n_row // 2
    nd = nd_own * n_row * n_col
    half = n_col * nd_own
    sem = pltpu.SemaphoreType.DMA
    vmem = pl.BlockSpec(memory_space=pltpu.VMEM)
    hbm = pl.BlockSpec(memory_space=pl.ANY)
    gq, gd, loss = pl.pallas_call(
        functools.partial(kernel, n_row, n_col, nd_own, nq * n_row * n_col),
        out_shape=(
            pltpu.VMEM((nq, width), BF16),
            pltpu.VMEM((nd_own, width), BF16),
            pltpu.VMEM((8, 128), F32),
        ),
        in_specs=[hbm, hbm, vmem, vmem, vmem],
        out_specs=(vmem, vmem, vmem),
        scratch_shapes=[
            pltpu.VMEM((nq, width), BF16),
            pltpu.VMEM((width, nq), BF16),
            pltpu.VMEM((nd, width), BF16),
            pltpu.VMEM((nd, nq), BF16),
            pltpu.VMEM((nd, width), F32),
            pltpu.VMEM((chips * half, width), F32),
            pltpu.VMEM((chips * half, width), F32),
            pltpu.VMEM((chips * nd_own, width), F32),
            pltpu.VMEM((1, nq), F32),
            pltpu.VMEM((3, 8, 128), F32),
            pltpu.VMEM((2, 8, 128), F32),
            pltpu.VMEM((n_col, 8, 128), F32),
            pltpu.VMEM((chips, 8, 128), F32),
            sem((2,)),
            sem((chips,)), sem((chips,)),
            sem((chips,)), sem((chips,)),
            sem((chips,)), sem((chips,)),
            sem((chips,)), sem((chips,)),
            sem((chips,)), sem((chips,)),
            sem((chips,)), sem((chips,)),
            sem((n_col + chips,)), sem((n_col + chips,)),
        ],
        compiler_params=pltpu.CompilerParams(
            collective_id=0, has_side_effects=True, vmem_limit_bytes=60 * 1024 * 1024
        ),
    )(
        queries, documents,
        log_norms.reshape(1, nq), weights.reshape(1, nq), positives.reshape(1, nq),
    )
    return (gq, gd, loss[0, 0])


def solution(mesh):
    placed = (
        P(("row", "col"), None),
        P(("row", "col"), None),
        P(("row", "col")),
        P(("row", "col")),
        P(("row", "col")),
    )
    return jax.shard_map(
        on_device,
        mesh=mesh,
        in_specs=placed,
        out_specs=(P(("row", "col"), None), P(("row", "col"), None), P()),
        check_vma=False,
    )
```

```python
import functools
import math

import jax
import jax.numpy as jnp
from jax import lax
from jax.experimental import pallas as pl
from jax.experimental.pallas import tpu as pltpu
from jax.sharding import PartitionSpec as P

MESH = pl.DeviceIdType.MESH
LOG2E = math.log2(math.e)
F32 = jnp.float32
BF16 = jnp.bfloat16


def flipped(index, step, size):
    total, bit = 0, 1
    while bit < size:
        own = (index // bit) % 2
        other = (step // bit) % 2
        total = total + bit * ((own + other) % 2)
        bit *= 2
    return total


def tree_sum(parts):
    while len(parts) > 1:
        parts = [parts[i] + parts[i + 1] for i in range(0, len(parts), 2)]
    return parts[0]


def kernel(
    n_row, n_col, nd_own, total_q,
    q_hbm, d_hbm, ln_ref, w_ref, pos_ref,
    gq_ref, gd_ref, loss_ref,
    q, q_t, docs, coeffs, part, recv2, recv3, bias, w2, pos2, ln2,
    gq_own, gq_out, gq_in, loss_own, loss_in,
    local_sem, s_z, r_z, s_c, r_c, s_2, r_2, s_3, r_3, s_l, r_l, s_q, r_q, s_g, r_g,
):
    chips = n_row // 2
    row = lax.axis_index("row")
    col = lax.axis_index("col")
    core = row % 2
    chip = row // 2
    nq, width = q_hbm.shape
    block = n_col * nd_own

    partner = (chip * 2 + (1 - core), col)
    along_row = [None] + [(flipped(chip, t, chips) * 2 + core, col) for t in range(1, chips)]
    along_col = [None] + [(row, flipped(col, s, n_col)) for s in range(1, n_col)]

    mine, theirs = pl.ds(0, nq), pl.ds(nq, nq)
    get_d = pltpu.make_async_copy(d_hbm, docs.at[pl.ds(0, nd_own)], local_sem.at[0])
    get_d.start()
    get_q = pltpu.make_async_copy(q_hbm, q.at[mine], local_sem.at[1])
    get_q.start()

    barrier = pltpu.get_barrier_semaphore()
    peers = [partner] + along_row[1:] + along_col[1:]
    for peer in peers:
        pl.semaphore_signal(barrier, inc=1, device_id=peer, device_id_type=MESH)
    get_d.wait()
    pl.semaphore_wait(barrier, len(peers))

    def send(src, dst, s_sem, r_sem, peer):
        return pltpu.make_async_remote_copy(
            src_ref=src, dst_ref=dst, send_sem=s_sem, recv_sem=r_sem,
            device_id=peer, device_id_type=MESH,
        )

    def piece(t, s, count=1):
        return docs.at[pl.ds(t * block + s * nd_own, count * nd_own)]

    started = []

    def go(copy):
        copy.start()
        started.append(copy)
        return copy

    def from_row(t):
        return send(piece(0, 0), piece(t, 0), s_z.at[t], r_z.at[t], along_row[t])

    def over_col(t):
        for s in range(1, n_col):
            send(piece(t, 0), piece(t, s), s_c.at[t], r_c.at[t], along_col[s]).start()

    def all_over_col(t):
        others = piece(t, 1, n_col - 1)
        return send(others, others, s_c.at[t], r_c.at[t], along_col[1])

    order = [0] + list(range(chips - 1, 0, -1))
    for t in order[1:]:
        go(from_row(t))
    over_col(0)

    shared = []
    for i, (own, both) in enumerate(((ln_ref, ln2), (w_ref, w2), (pos_ref, pos2))):
        shared.append(go(send(own, both.at[:, theirs], s_q.at[i], r_q.at[i], partner)))
        both[:, mine] = own[...]
    get_q.wait()
    q_copy = go(send(q.at[mine], q.at[theirs], s_q.at[3], r_q.at[3], partner))
    q_t[:, mine] = q[mine, :].T
    for c in shared:
        c.wait_recv()
    bias[...] = ln2[...] * LOG2E - jnp.log2(w2[...])
    q_copy.wait_recv()
    q_t[:, theirs] = q[theirs, :].T
    for t in order[1:]:
        from_row(t).wait_recv()
        over_col(t)

    iota = lax.broadcasted_iota(jnp.int32, (nd_own, 2 * nq), 0)

    def scores_of(t, acc):
        rows = pl.ds(t * block, block)
        sc = jnp.dot(docs[rows, :], q_t[...], preferred_element_type=F32)
        owner_row = flipped(chip, t, chips) * 2 + core
        for s in range(n_col):
            first = (owner_row * n_col + flipped(col, s, n_col)) * nd_own
            x = sc[s * nd_own:(s + 1) * nd_own, :]
            hit_w = jnp.where(pos2[...] - first == iota, w2[...], 0.0)
            co = jnp.exp2(x * (0.0625 * LOG2E) - bias[...]) - hit_w
            coeffs[pl.ds(t * block + s * nd_own, nd_own), :] = co.astype(BF16)
            acc = acc + jnp.sum((hit_w * x).reshape(nd_own // 8, 8, 2 * nq), axis=0)
        part[rows, :] = jnp.dot(coeffs[rows, :], q[...], preferred_element_type=F32)
        return acc

    def send_col(t):
        for s in range(1, n_col):
            at = pl.ds(t * block + s * nd_own, nd_own)
            send(part.at[at], recv2.at[at], s_2.at[t], r_2.at[t], along_col[s]).start()

    def all_col_sums(t):
        at = pl.ds(t * block + nd_own, (n_col - 1) * nd_own)
        return send(part.at[at], recv2.at[at], s_2.at[t], r_2.at[t], along_col[1])

    def row_copy(t):
        return send(
            part.at[pl.ds(t * block, nd_own)], recv3.at[pl.ds(t * nd_own, nd_own)],
            s_3.at[t], r_3.at[t], along_row[t],
        )

    def reduce_col(t):
        all_col_sums(t).wait_recv()
        total = part[pl.ds(t * block, nd_own), :]
        for s in range(1, n_col):
            total = total + recv2[pl.ds(t * block + s * nd_own, nd_own), :]
        part[pl.ds(t * block, nd_own), :] = total
        if t:
            go(row_copy(t))

    hit_sum = jnp.zeros((8, 2 * nq), F32)
    for i, t in enumerate(order):
        all_over_col(t).wait_recv()
        hit_sum = scores_of(t, hit_sum)
        send_col(t)
        if i >= 2:
            reduce_col(order[i - 2])

    hits = jnp.sum(jnp.sum(hit_sum, axis=0, keepdims=True), axis=1, keepdims=True)
    known = jnp.sum(w_ref[...] * ln_ref[...], axis=1, keepdims=True)
    loss_own[0] = jnp.broadcast_to(known - 0.0625 * hits, (8, 128))
    l_row = [
        go(send(loss_own.at[0], loss_in.at[t], s_l.at[t], r_l.at[t], along_row[t]))
        for t in range(1, chips)
    ]

    d_t = docs[...].T
    chunk = math.gcd(nq, 256)
    n_chunks = nq // chunk

    def query_gradient(first, j):
        at = pl.ds(first + j * chunk, chunk)
        return jnp.dot(d_t, coeffs[:, at], preferred_element_type=F32)

    g_copies = []
    for j in range(n_chunks):
        gq_out[j] = query_gradient(nq, j)
        g_copies.append(go(send(gq_out.at[j], gq_in.at[j], s_g.at[j], r_g.at[j], partner)))
    if chips > 1:
        reduce_col(order[-2])
    for j in range(n_chunks // 2):
        gq_own[j] = query_gradient(0, j)
    for c in l_row:
        c.wait_recv()
    loss_own[1] = tree_sum([loss_own[0]] + [loss_in[t] for t in range(1, chips)])
    l_col = [
        go(send(loss_own.at[1], loss_in.at[chips + s], s_l.at[chips + s], r_l.at[chips + s], along_col[s]))
        for s in range(1, n_col)
    ]
    reduce_col(order[-1])
    for j in range(n_chunks // 2, n_chunks):
        gq_own[j] = query_gradient(0, j)
    for j in range(n_chunks):
        g_copies[j].wait_recv()
        gq_ref[pl.ds(j * chunk, chunk), :] = ((gq_own[j] + gq_in[j]).T * 0.0625).astype(BF16)
    for c in l_col:
        c.wait_recv()
    loss_own[2] = tree_sum([loss_own[1]] + [loss_in[chips + s] for s in range(1, n_col)])
    l_pair = go(send(loss_own.at[2], loss_in.at[0], s_l.at[0], r_l.at[0], partner))
    total = part[pl.ds(0, nd_own), :]
    for t in order[1:]:
        row_copy(t).wait_recv()
        total = total + recv3[pl.ds(t * nd_own, nd_own), :]
    gd_ref[...] = (total * 0.0625).astype(BF16)
    l_pair.wait_recv()
    loss_ref[...] = (loss_own[2] + loss_in[0]) * (1.0 / total_q)

    for t in range(chips):
        all_over_col(t).wait_send()
        all_col_sums(t).wait_send()
    for copy in started:
        copy.wait_send()


def on_device(queries, documents, log_norms, weights, positives):
    n_row = lax.axis_size("row")
    n_col = lax.axis_size("col")
    nq, width = queries.shape
    nd_own = documents.shape[0]
    chips = n_row // 2
    nd = chips * n_col * nd_own
    chunk = math.gcd(nq, 256)
    n_chunks = nq // chunk
    sem = pltpu.SemaphoreType.DMA
    vmem = pl.BlockSpec(memory_space=pltpu.VMEM)
    hbm = pl.BlockSpec(memory_space=pl.ANY)
    gq, gd, loss = pl.pallas_call(
        functools.partial(kernel, n_row, n_col, nd_own, nq * n_row * n_col),
        out_shape=(
            pltpu.VMEM((nq, width), BF16),
            pltpu.VMEM((nd_own, width), BF16),
            pltpu.VMEM((8, 128), F32),
        ),
        in_specs=[hbm, hbm, vmem, vmem, vmem],
        out_specs=(vmem, vmem, vmem),
        scratch_shapes=[
            pltpu.VMEM((2 * nq, width), BF16),
            pltpu.VMEM((width, 2 * nq), BF16),
            pltpu.VMEM((nd, width), BF16),
            pltpu.VMEM((nd, 2 * nq), BF16),
            pltpu.VMEM((nd, width), F32),
            pltpu.VMEM((nd, width), F32),
            pltpu.VMEM((chips * nd_own, width), F32),
            pltpu.VMEM((1, 2 * nq), F32),
            pltpu.VMEM((1, 2 * nq), F32),
            pltpu.VMEM((1, 2 * nq), jnp.int32),
            pltpu.VMEM((1, 2 * nq), F32),
            pltpu.VMEM((n_chunks, width, chunk), F32),
            pltpu.VMEM((n_chunks, width, chunk), F32),
            pltpu.VMEM((n_chunks, width, chunk), F32),
            pltpu.VMEM((3, 8, 128), F32),
            pltpu.VMEM((chips + n_col, 8, 128), F32),
            sem((2,)),
        ] + [sem((chips,))] * 8 + [sem((chips + n_col,))] * 2 + [sem((4,))] * 2 + [sem((n_chunks,))] * 2,
        compiler_params=pltpu.CompilerParams(
            collective_id=0, has_side_effects=True, vmem_limit_bytes=60 * 1024 * 1024
        ),
    )(
        queries, documents,
        log_norms.reshape(1, nq), weights.reshape(1, nq), positives.reshape(1, nq),
    )
    return (gq, gd, loss[0, 0])


def solution(mesh):
    placed = (
        P(("row", "col"), None),
        P(("row", "col"), None),
        P(("row", "col")),
        P(("row", "col")),
        P(("row", "col")),
    )
    return jax.shard_map(
        on_device,
        mesh=mesh,
        in_specs=placed,
        out_specs=(P(("row", "col"), None), P(("row", "col"), None), P()),
        check_vma=False,
    )
```

```python
import functools
import math

import jax
import jax.numpy as jnp
from jax import lax
from jax.experimental import pallas as pl
from jax.experimental.pallas import tpu as pltpu
from jax.sharding import PartitionSpec as P

MESH = pl.DeviceIdType.MESH
LOG2E = math.log2(math.e)
F32 = jnp.float32
BF16 = jnp.bfloat16


def flipped(index, step, size):
    total, bit = 0, 1
    while bit < size:
        own = (index // bit) % 2
        other = (step // bit) % 2
        total = total + bit * ((own + other) % 2)
        bit *= 2
    return total


def tree_sum(parts):
    while len(parts) > 1:
        parts = [parts[i] + parts[i + 1] for i in range(0, len(parts), 2)]
    return parts[0]


def kernel(
    n_row, n_col, nd_own, total_q,
    q_hbm, d_hbm, ln_ref, w_ref, pos_ref,
    gq_ref, gd_ref, loss_ref,
    q, q_t, docs, coeffs, part, recv2, recv3, bias, w2, pos2, ln2,
    gq_own, gq_out, gq_in, loss_own, loss_in,
    local_sem, s_z, r_z, s_c, r_c, s_2, r_2, s_3, r_3, s_l, r_l, s_q, r_q, s_g, r_g,
):
    chips = n_row // 2
    row = lax.axis_index("row")
    col = lax.axis_index("col")
    core = row % 2
    chip = row // 2
    nq, width = q_hbm.shape
    block = n_col * nd_own

    partner = (chip * 2 + (1 - core), col)
    across = [(flipped(chip, t, chips) * 2 + (1 - core), col) for t in range(1, chips)]
    along_row = [None] + [(flipped(chip, t, chips) * 2 + core, col) for t in range(1, chips)]
    along_col = [None] + [(row, flipped(col, s, n_col)) for s in range(1, n_col)]

    mine, theirs = pl.ds(0, nq), pl.ds(nq, nq)
    get_d = pltpu.make_async_copy(d_hbm, docs.at[pl.ds(0, nd_own)], local_sem.at[0])
    get_d.start()
    get_q = pltpu.make_async_copy(q_hbm, q.at[mine], local_sem.at[1])
    get_q.start()

    barrier = pltpu.get_barrier_semaphore()
    peers = [partner] + along_row[1:] + across + along_col[1:]
    for peer in peers:
        pl.semaphore_signal(barrier, inc=1, device_id=peer, device_id_type=MESH)
    get_d.wait()
    pl.semaphore_wait(barrier, len(peers))

    def send(src, dst, s_sem, r_sem, peer):
        return pltpu.make_async_remote_copy(
            src_ref=src, dst_ref=dst, send_sem=s_sem, recv_sem=r_sem,
            device_id=peer, device_id_type=MESH,
        )

    def piece(t, s, count=1):
        return docs.at[pl.ds(t * block + s * nd_own, count * nd_own)]

    started = []

    def go(copy):
        copy.start()
        started.append(copy)
        return copy

    def from_row(t):
        return send(piece(0, 0), piece(t, 0), s_z.at[t], r_z.at[t], along_row[t])

    def over_col(t):
        for s in range(1, n_col):
            send(piece(t, 0), piece(t, s), s_c.at[t], r_c.at[t], along_col[s]).start()

    def all_over_col(t):
        others = piece(t, 1, n_col - 1)
        return send(others, others, s_c.at[t], r_c.at[t], along_col[1])

    order = [0] + list(range(chips - 1, 0, -1))
    for t in order[1:]:
        go(from_row(t))
    over_col(0)

    shared = []
    for i, (own, both) in enumerate(((ln_ref, ln2), (w_ref, w2), (pos_ref, pos2))):
        shared.append(go(send(own, both.at[:, theirs], s_q.at[i], r_q.at[i], partner)))
        both[:, mine] = own[...]
    get_q.wait()
    q_copy = go(send(q.at[mine], q.at[theirs], s_q.at[3], r_q.at[3], partner))
    q_t[:, mine] = q[mine, :].T
    for t in order[1:]:
        from_row(t).wait_recv()
        over_col(t)
    for c in shared:
        c.wait_recv()
    bias[...] = ln2[...] * LOG2E - jnp.log2(w2[...])
    q_copy.wait_recv()
    q_t[:, theirs] = q[theirs, :].T
    iota = lax.broadcasted_iota(jnp.int32, (nd_own, 2 * nq), 0)

    def coeffs_of(t, acc):
        rows = pl.ds(t * block, block)
        sc = jnp.dot(docs[rows, :], q_t[...], preferred_element_type=F32)
        owner_row = flipped(chip, t, chips) * 2 + core
        for s in range(n_col):
            first = (owner_row * n_col + flipped(col, s, n_col)) * nd_own
            x = sc[s * nd_own:(s + 1) * nd_own, :]
            hit_w = jnp.where(pos2[...] - first == iota, w2[...], 0.0)
            co = jnp.exp2(x * (0.0625 * LOG2E) - bias[...]) - hit_w
            coeffs[pl.ds(t * block + s * nd_own, nd_own), :] = co.astype(BF16)
            acc = acc + jnp.sum((hit_w * x).reshape(nd_own // 8, 8, 2 * nq), axis=0)
        return acc

    def document_sums(t):
        rows = pl.ds(t * block, block)
        part[rows, :] = jnp.dot(coeffs[rows, :], q[...], preferred_element_type=F32)

    def send_col(t):
        for s in range(1, n_col):
            at = pl.ds(t * block + s * nd_own, nd_own)
            send(part.at[at], recv2.at[at], s_2.at[t], r_2.at[t], along_col[s]).start()

    def all_col_sums(t):
        at = pl.ds(t * block + nd_own, (n_col - 1) * nd_own)
        return send(part.at[at], recv2.at[at], s_2.at[t], r_2.at[t], along_col[1])

    def row_copy(t):
        return send(
            part.at[pl.ds(t * block, nd_own)], recv3.at[pl.ds(t * nd_own, nd_own)],
            s_3.at[t], r_3.at[t], along_row[t],
        )

    def reduce_col(t):
        all_col_sums(t).wait_recv()
        total = part[pl.ds(t * block, nd_own), :]
        for s in range(1, n_col):
            total = total + recv2[pl.ds(t * block + s * nd_own, nd_own), :]
        part[pl.ds(t * block, nd_own), :] = total
        if t:
            go(row_copy(t))

    hit_sum = jnp.zeros((8, 2 * nq), F32)
    known = jnp.sum(w_ref[...] * ln_ref[...], axis=1, keepdims=True)
    row_group = [partner] + [peer for pair in zip(along_row[1:], across) for peer in pair]
    l_row = []
    for i, t in enumerate(order):
        all_over_col(t).wait_recv()
        hit_sum = coeffs_of(t, hit_sum)
        if i == chips - 1:
            hits = jnp.sum(jnp.sum(hit_sum, axis=0, keepdims=True), axis=1, keepdims=True)
            loss_own[0] = jnp.broadcast_to(known - 0.0625 * hits, (8, 128))
            for m, peer in reversed(list(enumerate(row_group, 1))):
                l_row.append(
                    go(send(loss_own.at[0], loss_in.at[m], s_l.at[m], r_l.at[m], peer))
                )
        document_sums(t)
        send_col(t)
        if i >= 2:
            reduce_col(order[i - 2])

    d_t = docs[...].T
    chunk = math.gcd(nq, 256)
    n_chunks = nq // chunk

    def query_gradient(first, j):
        at = pl.ds(first + j * chunk, chunk)
        return jnp.dot(d_t, coeffs[:, at], preferred_element_type=F32)

    g_copies = []
    for j in range(n_chunks):
        gq_out[j] = query_gradient(nq, j)
        g_copies.append(go(send(gq_out.at[j], gq_in.at[j], s_g.at[j], r_g.at[j], partner)))
    if chips > 1:
        reduce_col(order[-2])
    for j in range(n_chunks // 2):
        gq_own[j] = query_gradient(0, j)
    for c in l_row:
        c.wait_recv()
    loss_own[1] = tree_sum([loss_own[0]] + [loss_in[m] for m in range(1, n_row)])
    l_col = [
        go(send(loss_own.at[1], loss_in.at[n_row + s], s_l.at[n_row + s], r_l.at[n_row + s], along_col[s]))
        for s in range(1, n_col)
    ]
    reduce_col(order[-1])
    for j in range(n_chunks // 2, n_chunks):
        gq_own[j] = query_gradient(0, j)
    for j in range(n_chunks):
        g_copies[j].wait_recv()
        gq_ref[pl.ds(j * chunk, chunk), :] = ((gq_own[j] + gq_in[j]).T * 0.0625).astype(BF16)
    total = part[pl.ds(0, nd_own), :]
    for t in order[1:]:
        row_copy(t).wait_recv()
        total = total + recv3[pl.ds(t * nd_own, nd_own), :]
    gd_ref[...] = (total * 0.0625).astype(BF16)
    for c in l_col:
        c.wait_recv()
    loss_ref[...] = tree_sum([loss_own[1]] + [loss_in[n_row + s] for s in range(1, n_col)]) * (1.0 / total_q)

    for t in range(chips):
        all_over_col(t).wait_send()
        all_col_sums(t).wait_send()
    for copy in started:
        copy.wait_send()


def on_device(queries, documents, log_norms, weights, positives):
    n_row = lax.axis_size("row")
    n_col = lax.axis_size("col")
    nq, width = queries.shape
    nd_own = documents.shape[0]
    chips = n_row // 2
    nd = chips * n_col * nd_own
    chunk = math.gcd(nq, 256)
    n_chunks = nq // chunk
    sem = pltpu.SemaphoreType.DMA
    vmem = pl.BlockSpec(memory_space=pltpu.VMEM)
    hbm = pl.BlockSpec(memory_space=pl.ANY)
    gq, gd, loss = pl.pallas_call(
        functools.partial(kernel, n_row, n_col, nd_own, nq * n_row * n_col),
        out_shape=(
            pltpu.VMEM((nq, width), BF16),
            pltpu.VMEM((nd_own, width), BF16),
            pltpu.VMEM((8, 128), F32),
        ),
        in_specs=[hbm, hbm, vmem, vmem, vmem],
        out_specs=(vmem, vmem, vmem),
        scratch_shapes=[
            pltpu.VMEM((2 * nq, width), BF16),
            pltpu.VMEM((width, 2 * nq), BF16),
            pltpu.VMEM((nd, width), BF16),
            pltpu.VMEM((nd, 2 * nq), BF16),
            pltpu.VMEM((nd, width), F32),
            pltpu.VMEM((nd, width), F32),
            pltpu.VMEM((chips * nd_own, width), F32),
            pltpu.VMEM((1, 2 * nq), F32),
            pltpu.VMEM((1, 2 * nq), F32),
            pltpu.VMEM((1, 2 * nq), jnp.int32),
            pltpu.VMEM((1, 2 * nq), F32),
            pltpu.VMEM((n_chunks, width, chunk), F32),
            pltpu.VMEM((n_chunks, width, chunk), F32),
            pltpu.VMEM((n_chunks, width, chunk), F32),
            pltpu.VMEM((2, 8, 128), F32),
            pltpu.VMEM((n_row + n_col, 8, 128), F32),
            sem((2,)),
        ] + [sem((chips,))] * 8 + [sem((n_row + n_col,))] * 2 + [sem((4,))] * 2 + [sem((n_chunks,))] * 2,
        compiler_params=pltpu.CompilerParams(
            collective_id=0, has_side_effects=True, vmem_limit_bytes=60 * 1024 * 1024
        ),
    )(
        queries, documents,
        log_norms.reshape(1, nq), weights.reshape(1, nq), positives.reshape(1, nq),
    )
    return (gq, gd, loss[0, 0])


def solution(mesh):
    placed = (
        P(("row", "col"), None),
        P(("row", "col"), None),
        P(("row", "col")),
        P(("row", "col")),
        P(("row", "col")),
    )
    return jax.shard_map(
        on_device,
        mesh=mesh,
        in_specs=placed,
        out_specs=(P(("row", "col"), None), P(("row", "col"), None), P()),
        check_vma=False,
    )
```
